32 devices in a mesh: row: 8 (over z, core), col: 4 (over y, x).
Axes of the slice: x: 2, y: 2, z: 4, core: 2. Of those that a mesh axis runs over, the one named last changes fastest.
Arguments:
- design: float32 [4096, 65536], P('row', 'col'), may hold values from -0.0625 to 0.0625
- targets: float32 [32, 4096], P(None, 'row'), may hold values from -6 to 6
- warm_solution: float32 [32, 65536], P(None, ('col', 'row')), may hold values from -2 to 2
- warm_sparse: float32 [32, 65536], P(None, ('col', 'row')), may hold values from -2 to 2
- warm_dual: float32 [32, 65536], P(None, ('col', 'row')), may hold values from -1.5 to 1.5
- sparsity: float32 [32], replicated, may hold values from 0.02 to 0.2
Outputs:
- solution: float32 [32, 65536], P(None, ('col', 'row'))
- sparse: float32 [32, 65536], P(None, ('col', 'row'))
- scaled_dual: float32 [32, 65536], P(None, ('col', 'row'))
The draws below stay inside these ranges and needn't reach their ends.
All inputs are finite; a program needn't handle non-finite values.
Results may differ from the reference program's by a relative error of at most 0.0003.
Values sent between devices are 32-bit elements; how exact they have to be, the bound alone decides.
A program may use at most 128 MiB of HBM per device.

```python
import math
import jax
import jax.numpy as jnp
from jax import lax

N = 65536
K = 32
OUTER = 1
STEPS = 3
M = 4096


def strengthened(array, rng, source, target, shards_of, factor):
    owner, partner = [(jnp.arange(array.shape[position]) // (array.shape[position] // shards_of)).reshape([-1 if axis == position else 1 for axis in range(array.ndim)]) for position in (source, target)]
    chosen = jax.random.permutation(rng, shards_of)[partner]
    strong = (owner == chosen) | (owner == (partner + shards_of // 2) % shards_of)
    return jnp.where(strong, factor * array, array)


def block_scale(own_key, shape, pieces, least, top_value):
    def one(axis_at, shards_of):
        draws = jax.random.uniform(jax.random.fold_in(jax.random.fold_in(own_key, 6), axis_at), (shards_of,), jnp.float32, least / len(pieces), top_value / len(pieces))
        return jnp.repeat(jnp.exp(draws), shape[axis_at] // shards_of).reshape((-1,) + (1,) * (len(shape) - axis_at - 1))

    level = one(*pieces[0])
    for cut in pieces[1:]:
        level = level * one(*cut)
    return level


def bell_draw(stream_key, dims, deviation, limit, shards=(), dtype=jnp.bfloat16):
    array = jax.random.normal(stream_key, dims, jnp.float32) * deviation
    if len(shards) > 0:
        array = block_scale(stream_key, dims, shards, -0.22, 0.18) * array
    return jnp.clip(array, min=-limit, max=limit).astype(dtype)


def heavy_noise(stream_key, dims, spread, limit, split, heavy, dtype=jnp.bfloat16):
    values = spread * jax.random.normal(stream_key, dims, jnp.float32)
    if split:
        values = values * block_scale(stream_key, dims, split, -0.22, 0.18)
    return jnp.clip(strengthened(values, jax.random.fold_in(stream_key, 3), *heavy), -limit, limit).astype(dtype)


def setup_inputs(seed: int = 0) -> dict:
    key_list = jax.random.split(jax.random.key(seed), 7)
    design = heavy_noise(key_list[0], (M, N), (N // 4) ** -0.5, 0.0625, ((0, 8), (1, 4)), (0, 1, 8, 2.0), jnp.float32)
    targets = bell_draw(key_list[1], (K, M), 1.0, 6.0, ((1, 8),), jnp.float32)
    warm_solution = bell_draw(key_list[2], (K, N), 0.3, 2.0, ((1, 32),), jnp.float32)
    warm_sparse = bell_draw(key_list[3], (K, N), 0.3, 2.0, ((1, 32),), jnp.float32)
    warm_dual = bell_draw(key_list[4], (K, N), 0.2, 1.5, ((1, 32),), jnp.float32)
    sparsity = jnp.clip(jnp.exp(jax.random.uniform(key_list[5], (K,), jnp.float32, math.log(0.02), math.log(0.2))), 0.02, 0.2)
    return dict(design=design, targets=targets, warm_solution=warm_solution, warm_sparse=warm_sparse, warm_dual=warm_dual, sparsity=sparsity)


penalty = 0.5


def gram(design, vector):
    forward = lax.dot_general(vector, design, (((1,), (1,)), ((), ())), precision=lax.Precision.HIGHEST, preferred_element_type=jnp.float32)
    back = jnp.dot(forward, design, precision=lax.Precision.HIGHEST, preferred_element_type=jnp.float32)
    return back + penalty * vector


def reference(design, targets, warm_solution, warm_sparse, warm_dual, sparsity):
    fitted = jnp.dot(targets, design, precision=lax.Precision.HIGHEST, preferred_element_type=jnp.float32)
    thresh = (sparsity / penalty)[:, None]
    solution, sparse, scaled_dual = warm_solution, warm_sparse, warm_dual
    for outer in range(OUTER):
        rhs = fitted + penalty * (sparse - scaled_dual)
        residual = rhs - gram(design, solution)
        direction = residual
        norm_now = jnp.sum(residual * residual, axis=1, keepdims=True)
        for step in range(STEPS):
            image = gram(design, direction)
            alpha = norm_now / jnp.sum(direction * image, axis=1, keepdims=True)
            solution = solution + alpha * direction
            residual = residual - alpha * image
            norm_next = jnp.sum(residual * residual, axis=1, keepdims=True)
            direction = residual + (norm_next / norm_now) * direction
            norm_now = norm_next
        merged = solution + scaled_dual
        sparse = jnp.sign(merged) * jnp.maximum(jnp.abs(merged) - thresh, 0.0)
        scaled_dual = merged - sparse
    return solution, sparse, scaled_dual
```

```python
import functools

import jax
import jax.numpy as jnp
from jax import lax
from jax.experimental import pallas as pl
from jax.experimental.pallas import tpu as pltpu
from jax.sharding import PartitionSpec as P

STEPS = 3
GROUPS = 2
CHUNKS = 8
HOP = 2
GATHER = 2
SHARE = 3
LANES = 128
MESH = pl.DeviceIdType.MESH

penalty = 0.5


def halves(values):
    top = values.astype(jnp.bfloat16)
    return top, (values - top.astype(jnp.float32)).astype(jnp.bfloat16)


def dot(left, right, dims):
    return lax.dot_general(left, right, (dims, ((), ())), preferred_element_type=jnp.float32)


def lane_sums(values):
    total = values[:, :LANES]
    for at in range(LANES, values.shape[1], LANES):
        total = total + values[:, at:at + LANES]
    return total


def row_sums(values):
    return jnp.sum(values, axis=1, keepdims=True)


def admm_kernel(
    nr, nc, period,
    design_ref, targets_ref, x_ref, sparse_ref, dual_ref, out_ref,
    high, low, stage, resid, direct, seen, acc, norms, scale,
    part, part_land, right_in, left_in, right_out, left_out, total,
    mine, land, stat, stat_land,
    load_sem, gather_send, gather_recv, across_send, across_recv,
    part_send, part_recv, total_send, total_recv,
    right_send, right_recv, left_send, left_recv,
    col_send, col_recv, row_send, row_recv,
):
    row, col = lax.axis_index("row"), lax.axis_index("col")
    line = nr // 2
    z, core = row // 2, row % 2
    other = 1 - core
    depth, features = high.shape
    rows, width = x_ref.shape
    few = rows // GROUPS
    chunk = features // CHUNKS
    half = chunk // 2
    phases = STEPS * GROUPS
    last_z = line - 1

    def own(slot):
        return pl.ds(pl.multiple_of(slot * width, LANES), width)

    def remote(source, target, send, recv, where):
        return pltpu.make_async_remote_copy(
            src_ref=source, dst_ref=target, send_sem=send, recv_sem=recv,
            device_id=where, device_id_type=MESH,
        )

    near = jnp.minimum(z, last_z - z)
    far_sign = jnp.where(z < last_z - z, 1, -1)

    def origin_at(k):
        paired = k <= 2 * near
        distance = jnp.where(paired, (k + 1) // 2, k - near)
        sign = jnp.where(paired, 1 - 2 * (k % 2), far_sign)
        return z + sign * distance, sign

    def slot_at(n):
        origin, _ = origin_at(n // 2)
        return origin * 2 + jnp.where(n % 2 == 0, core, other)

    def piece_at(m):
        at = slot_at(m // 2) * width + (m % 2) * (width // 2)
        return pl.ds(pl.multiple_of(at, LANES), width // 2)

    def load(m):
        buffer = m % 2
        return pltpu.make_async_copy(
            design_ref.at[:, piece_at(m)], stage.at[buffer], load_sem.at[buffer]
        )

    def pass_on(source, origin, sign, at):
        return remote(
            source, resid.at[:, own(origin * 2 + core)], gather_send.at[at],
            gather_recv.at[origin], {"row": (z + sign) * 2 + core},
        )

    def across(source, origin):
        return remote(
            source, resid.at[:, own(origin * 2 + core)], across_send.at[origin],
            across_recv.at[origin], {"row": z * 2 + other},
        )

    def arrived(origin):
        cols = own(origin * 2 + other)
        return remote(
            resid.at[:, cols], resid.at[:, cols], across_send.at[origin],
            across_recv.at[origin], {"row": z * 2 + other},
        )

    load(0).start()
    load(1).start()

    barrier = pltpu.get_barrier_semaphore()

    @pl.loop(1, nc)
    def _(s):
        pl.semaphore_signal(
            barrier, inc=1, device_id={"col": lax.rem(col + s, nc)}, device_id_type=MESH
        )

    @pl.loop(1, nr)
    def _(s):
        pl.semaphore_signal(
            barrier, inc=1, device_id={"row": lax.rem(row + s, nr)}, device_id_type=MESH
        )

    pl.semaphore_wait(barrier, nc + nr - 2)

    for i, sign in enumerate((1, -1)):

        @pl.when(jnp.logical_and(z + sign >= 0, z + sign < line))
        def _():
            pass_on(x_ref, z, sign, line + i).start()

    across(x_ref, z).start()
    resid[:, own(row)] = x_ref[...]
    out_ref[...] = x_ref[...]
    direct[...] = jnp.zeros_like(direct)
    direct[:, own(row)] = penalty * ((sparse_ref[...] - dual_ref[...]) - x_ref[...])
    acc[...] = jnp.zeros_like(acc)
    scale[0] = jnp.full_like(scale[0], -1.0)
    for i in range(1, 4):
        scale[i] = jnp.zeros_like(scale[i])

    @pl.when(z == 0)
    def _():
        right_in[...] = jnp.zeros_like(right_in)

    @pl.when(z == last_z)
    def _():
        left_in[...] = jnp.zeros_like(left_in)

    def take(n):
        for m in (2 * n, 2 * n + 1):
            load(m).wait()
            top, rest = halves(stage[m % 2])
            high[:, piece_at(m)] = top
            low[:, piece_at(m)] = rest

            @pl.when(m + 2 < 2 * nr)
            def _():
                load(m + 2).start()

    def add_seen(cols):
        top, rest = halves(resid[:, cols])
        acc[: 2 * rows] += dot(jnp.concatenate([top, rest], axis=0), high[:, cols], ((1,), (1,)))
        acc[2 * rows:] += dot(top, low[:, cols], ((1,), (1,)))

    @pl.loop(0, line)
    def _(k):
        origin, sign = origin_at(k)
        take(2 * k)

        @pl.when(k > 0)
        def _():
            here = own(origin * 2 + core)
            piece = resid.at[:, here]
            onward = jnp.logical_and(z - sign >= 0, z - sign < line)
            pass_on(piece, origin, sign, origin).wait_recv()

            @pl.when(onward)
            def _():
                pass_on(piece, origin, -sign, origin).start()

            across(piece, origin).start()

        add_seen(own(origin * 2 + core))
        take(2 * k + 1)
        arrived(origin).wait_recv()
        add_seen(own(origin * 2 + other))

    @pl.loop(0, line)
    def _(k):
        origin, sign = origin_at(k)
        across(x_ref, origin).wait_send()

        @pl.when(jnp.logical_and(k > 0, jnp.logical_and(z - sign >= 0, z - sign < line)))
        def _():
            pass_on(x_ref, origin, -sign, origin).wait_send()

    for i, sign in enumerate((1, -1)):

        @pl.when(jnp.logical_and(z + sign >= 0, z + sign < line))
        def _():
            pass_on(x_ref, z, sign, line + i).wait_send()

    def to_cols(slot, s):
        return remote(
            mine.at[slot], land.at[slot, col], col_send.at[slot, s], col_recv.at[slot, s],
            {"col": lax.rem(col + s, nc)},
        )

    def summed(slot):
        values = land[slot, 0]
        for s in range(1, nc):
            values = values + land[slot, s]
        return values

    def send_cols(slot):
        land[slot, col] = mine[slot]

        @pl.loop(1, nc)
        def _(s):
            to_cols(slot, s).start()

    def wait_cols(slot):
        @pl.loop(1, nc)
        def _(s):
            to_cols(slot, s).wait()

    seen_first = acc[:rows] + (acc[rows:2 * rows] + acc[2 * rows:])
    for g in range(GROUPS):
        slot = phases + g
        mine[slot, :, :depth] = seen_first[g * few:(g + 1) * few]
        mine[slot, :, depth:] = jnp.zeros((few, LANES), jnp.float32)
        send_cols(slot)
    for g in range(GROUPS):
        slot = phases + g
        wait_cols(slot)
        seen[g] = targets_ref[g * few:(g + 1) * few] - summed(slot)[:, :depth]

    def pair(source, target, send, recv):
        return remote(source, target, send, recv, {"row": z * 2 + other})

    def part_copy(b, j):
        return pair(
            part.at[b, j, other], part_land.at[b, j], part_send.at[b, j], part_recv.at[b, j]
        )

    def total_copy(b, j):
        return pair(
            total.at[b, j, core], total.at[b, j, core], total_send.at[b, j], total_recv.at[b, j]
        )

    def right_copy(b, j):
        return remote(
            right_out.at[b, j], right_in.at[b, j], right_send.at[b, j], right_recv.at[b, j],
            {"row": (z + 1) * 2 + core},
        )

    def left_copy(b, j):
        return remote(
            left_out.at[b, j], left_in.at[b, j], left_send.at[b, j], left_recv.at[b, j],
            {"row": (z - 1) * 2 + core},
        )

    def row_copy(p, s):
        return remote(
            stat.at[p], stat_land.at[p, row], row_send.at[p, s], row_recv.at[p, s],
            {"row": lax.rem(row + s, nr)},
        )

    def columns(j):
        return pl.ds(pl.multiple_of(j * chunk, LANES), chunk)

    reach = 2 + HOP * last_z
    ended = CHUNKS - 1 + reach + GATHER

    def run(t):
        def task(delay, body):
            u = t - delay
            p, j = lax.div(u, period), lax.rem(u, period)
            live = jnp.logical_and(u >= 0, jnp.logical_and(p < phases, j < CHUNKS))

            @pl.when(live)
            def _():
                body(p, lax.rem(p, 2), lax.rem(p, GROUPS), j)

        def once(delay, body):
            u = t - delay
            p = lax.div(u, period)
            live = jnp.logical_and(u >= 0, jnp.logical_and(p < phases, lax.rem(u, period) == 0))

            @pl.when(live)
            def _():
                body(p, lax.rem(p, GROUPS))

        def step_size(p, g):
            @pl.loop(1, nr)
            def _(s):
                row_copy(p, s).wait()

            square = stat_land[p, 0]
            for s in range(1, nr):
                square = square + stat_land[p, s]
            alpha = scale[3, g] / (square + penalty * scale[2, g])
            scale[0, g] = alpha
            mine_rows = pl.ds(pl.multiple_of(g * few, 8), few)
            along = resid[mine_rows, own(row)] + scale[1, g][:, :1] * direct[mine_rows, own(row)]
            out_ref[mine_rows, :] += alpha[:, :1] * along

        def gathered(p, g):
            wait_cols(p)
            values = summed(p)
            told = values[:, depth:]
            norm, cross = told[:, :1], told[:, LANES - 1:]
            start = p < GROUPS
            before = jnp.where(start, norm, scale[3, g][:, :1])
            ratio = jnp.where(start, 0.0, norm / before)
            length = norm + ratio * (2.0 * cross + ratio * scale[2, g][:, :1])
            image = values[:, :depth] + ratio * seen[g]
            seen[g] = image
            wide = (few, LANES)
            scale[1, g] = jnp.broadcast_to(ratio, wide)
            scale[2, g] = jnp.broadcast_to(length, wide)
            scale[3, g] = jnp.broadcast_to(norm, wide)
            square = jnp.broadcast_to(row_sums(image * image), wide)
            stat[p] = square
            stat_land[p, row] = square

            @pl.loop(1, nr)
            def _(s):
                row_copy(p, s).start()

        def reduced(p, b, g, j):
            part_copy(b, j).wait()
            part[b, j, core] = part[b, j, core] + part_land[b, j]

        def rightward(p, b, g, j):
            @pl.when(z > 0)
            def _():
                right_copy(b, j).wait_recv()

            @pl.when(z < last_z)
            def _():
                right_out[b, j] = right_in[b, j] + part[b, j, core]
                right_copy(b, j).start()

        def leftward(p, b, g, j):
            @pl.when(z < last_z)
            def _():
                left_copy(b, j).wait_recv()

            @pl.when(z > 0)
            def _():
                left_out[b, j] = left_in[b, j] + part[b, j, core]
                left_copy(b, j).start()

        def joined(p, b, g, j):
            total[b, j, core] = (right_in[b, j] + part[b, j, core]) + left_in[b, j]
            total_copy(b, j).start()

        def spread_back(p, b, g, j):
            cols = columns(j)
            top, rest = halves(seen[g])
            both = dot(jnp.concatenate([top, rest], axis=0), high[:, cols], ((1,), (0,)))
            values = both[:few] + (both[few:] + dot(top, low[:, cols], ((1,), (0,))))
            part[b, j, 0] = values[:, :half]
            part[b, j, 1] = values[:, half:]

            @pl.when(p < GROUPS)
            def _():
                mine_rows = pl.ds(pl.multiple_of(g * few, 8), few)
                held = direct[mine_rows, cols]
                part[b, j, 0] += held[:, :half]
                part[b, j, 1] += held[:, half:]

            part_copy(b, j).start()

        def product(p, b, g, j):
            total_copy(b, j).wait_send()
            pair(
                total.at[b, j, other], total.at[b, j, other],
                total_send.at[b, j], total_recv.at[b, j],
            ).wait_recv()

            @pl.when(z < last_z)
            def _():
                right_copy(b, j).wait_send()

            @pl.when(z > 0)
            def _():
                left_copy(b, j).wait_send()

            cols = columns(j)
            mine_rows = pl.ds(pl.multiple_of(g * few, 8), few)
            image = jnp.concatenate([total[b, j, 0], total[b, j, 1]], axis=1)
            kept = jnp.where(p < GROUPS, 0.0, 1.0)
            before = resid[mine_rows, cols] * kept
            along = before + scale[1, g][:, :1] * direct[mine_rows, cols]
            after = before - scale[0, g][:, :1] * (image + penalty * along)
            resid[mine_rows, cols] = after
            direct[mine_rows, cols] = along

            @pl.when(j == 0)
            def _():
                norms[...] = jnp.zeros_like(norms)
                acc[: 3 * few] = jnp.zeros((3 * few, depth), jnp.float32)

            norms[0] += lane_sums(after * after)
            norms[1] += lane_sums(after * along)
            top, rest = halves(after)
            acc[: 2 * few] += dot(
                jnp.concatenate([top, rest], axis=0), high[:, cols], ((1,), (1,))
            )
            acc[2 * few:3 * few] += dot(top, low[:, cols], ((1,), (1,)))

            @pl.when(j == CHUNKS - 1)
            def _():
                mine[p, :, :depth] = acc[:few] + (acc[few:2 * few] + acc[2 * few:3 * few])
                lane = lax.broadcasted_iota(jnp.int32, (few, LANES), 1)
                mine[p, :, depth:] = jnp.where(
                    lane < LANES // 2, row_sums(norms[0]), row_sums(norms[1])
                )
                send_cols(p)

        once(ended + SHARE, step_size)
        once(ended, gathered)
        task(1, reduced)
        task(1 + HOP * z, rightward)
        task(1 + HOP * (last_z - z), leftward)
        task(1 + HOP * jnp.maximum(z, last_z - z), joined)
        task(0, spread_back)
        task(reach, product)

    pl.loop(0, (phases - 1) * period + ended + SHARE + 1)(run)


def solution(mesh):
    nr, nc = mesh.shape["row"], mesh.shape["col"]
    line = nr // 2

    def solve(design, targets, x, sparse, dual):
        depth, features = design.shape
        rows, width = x.shape
        few, half = rows // GROUPS, features // CHUNKS // 2
        phases = STEPS * GROUPS
        ended = CHUNKS - 1 + 2 + HOP * (line - 1) + GATHER
        period = max(CHUNKS, -(-ended // GROUPS))
        vmem = pl.BlockSpec(memory_space=pltpu.VMEM)
        hbm = pl.BlockSpec(memory_space=pl.ANY)
        f32 = jnp.float32
        dma = pltpu.SemaphoreType.DMA
        step = (2, CHUNKS)
        return pl.pallas_call(
            functools.partial(admm_kernel, nr, nc, period),
            out_shape=jax.ShapeDtypeStruct((rows, width), f32),
            in_specs=[hbm, vmem, vmem, vmem, vmem],
            out_specs=vmem,
            scratch_shapes=[
                pltpu.VMEM((depth, features), jnp.bfloat16),
                pltpu.VMEM((depth, features), jnp.bfloat16),
                pltpu.VMEM((2, depth, width // 2), f32),
                pltpu.VMEM((rows, features), f32),
                pltpu.VMEM((rows, features), f32),
                pltpu.VMEM((GROUPS, few, depth), f32),
                pltpu.VMEM((3 * rows, depth), f32),
                pltpu.VMEM((2, few, LANES), f32),
                pltpu.VMEM((4, GROUPS, few, LANES), f32),
                pltpu.VMEM(step + (2, few, half), f32),
                pltpu.VMEM(step + (few, half), f32),
                pltpu.VMEM(step + (few, half), f32),
                pltpu.VMEM(step + (few, half), f32),
                pltpu.VMEM(step + (few, half), f32),
                pltpu.VMEM(step + (few, half), f32),
                pltpu.VMEM(step + (2, few, half), f32),
                pltpu.VMEM((phases + GROUPS, few, depth + LANES), f32),
                pltpu.VMEM((phases + GROUPS, nc, few, depth + LANES), f32),
                pltpu.VMEM((phases, few, LANES), f32),
                pltpu.VMEM((phases, nr, few, LANES), f32),
                dma((2,)),
                dma((line + 2,)),
                dma((line,)),
                dma((line,)),
                dma((line,)),
                dma(step), dma(step), dma(step), dma(step),
                dma(step), dma(step), dma(step), dma(step),
                dma((phases + GROUPS, nc)),
                dma((phases + GROUPS, nc)),
                dma((phases, nr)),
                dma((phases, nr)),
            ],
            compiler_params=pltpu.CompilerParams(
                collective_id=0, has_side_effects=True, vmem_limit_bytes=60 * 1024 * 1024
            ),
        )(design, targets, x, sparse, dual)

    def on_device(design, targets, warm_solution, warm_sparse, warm_dual, sparsity):
        solution = solve(design, targets, warm_solution, warm_sparse, warm_dual)
        thresh = (sparsity / penalty)[:, None]
        merged = solution + warm_dual
        sparse = jnp.sign(merged) * jnp.maximum(jnp.abs(merged) - thresh, 0.0)
        return solution, sparse, merged - sparse

    vector = P(None, ("col", "row"))
    return jax.shard_map(
        on_device,
        mesh=mesh,
        in_specs=(P("row", "col"), P(None, "row"), vector, vector, vector, P()),
        out_specs=(vector, vector, vector),
        check_vma=False,
    )
```

```python
import functools

import jax
import jax.numpy as jnp
from jax import lax
from jax.experimental import pallas as pl
from jax.experimental.pallas import tpu as pltpu
from jax.sharding import PartitionSpec as P

STEPS = 3
CHUNKS = 16
PARTS = 2
HOP = 2
SHARE = 3
LANES = 128
VMEM_LIMIT = 60 * 1024 * 1024
MESH = pl.DeviceIdType.MESH

penalty = 0.5


def halves(values):
    top = values.astype(jnp.bfloat16)
    return top, (values - top.astype(jnp.float32)).astype(jnp.bfloat16)


def dot(left, right, dims):
    return lax.dot_general(left, right, (dims, ((), ())), preferred_element_type=jnp.float32)


def lane_sums(values):
    total = values[:, :LANES]
    for at in range(LANES, values.shape[1], LANES):
        total = total + values[:, at:at + LANES]
    return total


def row_sums(values):
    return jnp.sum(values, axis=1, keepdims=True)


def admm_kernel(
    nr, nc, chunks,
    design_ref, targets_ref, x_ref, sparse_ref, dual_ref, out_ref, step_ref,
    high, low, stage, resid, direct, seen, acc, norms, scale,
    part, part_land, right_in, left_in, right_out, left_out, total,
    mine, land, stat, stat_land,
    load_sem, gather_send, gather_recv, across_send, across_recv,
    part_send, part_recv, total_send, total_recv,
    right_send, right_recv, left_send, left_recv,
    col_send, col_recv, row_send, row_recv,
):
    row, col = lax.axis_index("row"), lax.axis_index("col")
    line = nr // 2
    z, core = row // 2, row % 2
    other = 1 - core
    depth, features = high.shape
    rows, width = x_ref.shape
    chunk = features // chunks
    half = chunk // 2
    piece = half // PARTS
    bit = width // 2
    last_z = line - 1
    reach = 2 + HOP * last_z

    def own(slot):
        return pl.ds(pl.multiple_of(slot * width, LANES), width)

    def bits(slot, h):
        return pl.ds(pl.multiple_of(slot * width + h * bit, LANES), bit)

    def remote(source, target, send, recv, where):
        return pltpu.make_async_remote_copy(
            src_ref=source, dst_ref=target, send_sem=send, recv_sem=recv,
            device_id=where, device_id_type=MESH,
        )

    near = jnp.minimum(z, last_z - z)
    far_sign = jnp.where(z < last_z - z, 1, -1)

    def origin_at(k):
        paired = k <= 2 * near
        distance = jnp.where(paired, (k + 1) // 2, k - near)
        sign = jnp.where(paired, 1 - 2 * (k % 2), far_sign)
        return z + sign * distance, sign

    def slot_at(n):
        origin, _ = origin_at(n // 2)
        return origin * 2 + jnp.where(n % 2 == 0, core, other)

    def load(m):
        buffer = m % 2
        return pltpu.make_async_copy(
            design_ref.at[:, bits(slot_at(m // 2), m % 2)], stage.at[buffer], load_sem.at[buffer]
        )

    def along_line(source, origin, h, sign, at):
        return remote(
            source, resid.at[:, bits(origin * 2 + core, h)], gather_send.at[at, h],
            gather_recv.at[origin, h], {"row": (z + sign) * 2 + core},
        )

    def across(source, origin, h):
        return remote(
            source, resid.at[:, bits(origin * 2 + core, h)], across_send.at[origin, h],
            across_recv.at[origin, h], {"row": z * 2 + other},
        )

    def arrived(origin, h):
        where = resid.at[:, bits(origin * 2 + other, h)]
        return remote(
            where, where, across_send.at[origin, h], across_recv.at[origin, h],
            {"row": z * 2 + other},
        )

    def inside(place):
        return jnp.logical_and(place >= 0, place < line)

    load(0).start()
    load(1).start()

    barrier = pltpu.get_barrier_semaphore()

    @pl.loop(1, nc)
    def _(s):
        pl.semaphore_signal(
            barrier, inc=1, device_id={"col": lax.rem(col + s, nc)}, device_id_type=MESH
        )

    @pl.loop(1, nr)
    def _(s):
        pl.semaphore_signal(
            barrier, inc=1, device_id={"row": lax.rem(row + s, nr)}, device_id_type=MESH
        )

    resid[:, own(row)] = x_ref[...]
    out_ref[...] = x_ref[...]
    direct[...] = jnp.zeros_like(direct)
    direct[:, own(row)] = penalty * ((sparse_ref[...] - dual_ref[...]) - x_ref[...])
    acc[...] = jnp.zeros_like(acc)
    scale[0] = jnp.full_like(scale[0], -1.0)
    for i in range(1, 4):
        scale[i] = jnp.zeros_like(scale[i])

    @pl.when(z == 0)
    def _():
        right_in[...] = jnp.zeros_like(right_in)

    @pl.when(z == last_z)
    def _():
        left_in[...] = jnp.zeros_like(left_in)

    pl.semaphore_wait(barrier, nc + nr - 2)

    for h in range(2):
        source = x_ref.at[:, pl.ds(h * bit, bit)]
        for i, sign in enumerate((1, -1)):

            @pl.when(inside(z + sign))
            def _():
                along_line(source, z, h, sign, line + i).start()

        across(source, z, h).start()

    def take(m):
        load(m).wait()
        top, rest = halves(stage[m % 2])
        cols = bits(slot_at(m // 2), m % 2)
        high[:, cols] = top
        low[:, cols] = rest

        @pl.when(m + 2 < 2 * nr)
        def _():
            load(m + 2).start()

    def add_seen(slot):
        cols = own(slot)
        top, rest = halves(resid[:, cols])
        acc[: 2 * rows] += dot(jnp.concatenate([top, rest], axis=0), high[:, cols], ((1,), (1,)))
        acc[2 * rows:] += dot(top, low[:, cols], ((1,), (1,)))

    @pl.loop(0, line)
    def _(k):
        origin, sign = origin_at(k)
        for h in range(2):
            take(4 * k + h)

            @pl.when(k > 0)
            def _():
                held = resid.at[:, bits(origin * 2 + core, h)]
                along_line(held, origin, h, sign, origin).wait_recv()

                @pl.when(inside(z - sign))
                def _():
                    along_line(held, origin, h, -sign, origin).start()

                across(held, origin, h).start()

        add_seen(origin * 2 + core)
        for h in range(2):
            take(4 * k + 2 + h)
            arrived(origin, h).wait_recv()
        add_seen(origin * 2 + other)

    @pl.loop(0, line)
    def _(k):
        origin, sign = origin_at(k)
        for h in range(2):
            source = x_ref.at[:, pl.ds(h * bit, bit)]
            across(source, origin, h).wait_send()

            @pl.when(jnp.logical_and(k > 0, inside(z - sign)))
            def _():
                along_line(source, origin, h, -sign, origin).wait_send()

    for h in range(2):
        source = x_ref.at[:, pl.ds(h * bit, bit)]
        for i, sign in enumerate((1, -1)):

            @pl.when(inside(z + sign))
            def _():
                along_line(source, z, h, sign, line + i).wait_send()

    def to_cols(slot, s):
        return remote(
            mine.at[slot], land.at[slot, col], col_send.at[slot, s], col_recv.at[slot, s],
            {"col": lax.rem(col + s, nc)},
        )

    def summed(slot):
        @pl.loop(1, nc)
        def _(s):
            to_cols(slot, s).wait()

        values = land[slot, 0]
        for s in range(1, nc):
            values = values + land[slot, s]
        return values

    def send_cols(slot, told):
        mine[slot, :, :depth] = acc[:rows] + (acc[rows:2 * rows] + acc[2 * rows:])
        mine[slot, :, depth:] = told
        land[slot, col] = mine[slot]

        @pl.loop(1, nc)
        def _(s):
            to_cols(slot, s).start()

    send_cols(STEPS, jnp.zeros((rows, LANES), jnp.float32))
    seen[...] = targets_ref[...] - summed(STEPS)[:, :depth]

    def pair(source, target, send, recv):
        return remote(source, target, send, recv, {"row": z * 2 + other})

    def part_copy(j, a):
        return pair(
            part.at[j, other, a], part_land.at[j, a],
            part_send.at[j, a], part_recv.at[j, a],
        )

    def total_copy(j, a, side):
        where = total.at[j, side, a]
        return pair(where, where, total_send.at[j, a], total_recv.at[j, a])

    def right_copy(b, j, a):
        return remote(
            right_out.at[j, a], right_in.at[b, j, a],
            right_send.at[j, a], right_recv.at[b, j, a], {"row": (z + 1) * 2 + core},
        )

    def left_copy(b, j, a):
        return remote(
            left_out.at[j, a], left_in.at[b, j, a],
            left_send.at[j, a], left_recv.at[b, j, a], {"row": (z - 1) * 2 + core},
        )

    def row_copy(p, s):
        return remote(
            stat.at[p], stat_land.at[p, row], row_send.at[p, s], row_recv.at[p, s],
            {"row": lax.rem(row + s, nr)},
        )

    def columns(j):
        return pl.ds(pl.multiple_of(j * chunk, LANES), chunk)

    def step_size(p):
        @pl.loop(1, nr)
        def _(s):
            row_copy(p, s).wait()

        square = stat_land[p, 0]
        for s in range(1, nr):
            square = square + stat_land[p, s]
        alpha = scale[3] / (square + penalty * scale[2])
        scale[0] = alpha
        along = resid[:, own(row)] + scale[1][:, :1] * direct[:, own(row)]
        return alpha[:, :1] * along

    def gathered(p):
        values = summed(p)
        told = values[:, depth:]
        norm, cross = told[:, :1], told[:, LANES - 1:]
        start = p == 0
        before = jnp.where(start, norm, scale[3][:, :1])
        ratio = jnp.where(start, 0.0, norm / before)
        length = norm + ratio * (2.0 * cross + ratio * scale[2][:, :1])
        image = values[:, :depth] + ratio * seen[...]
        seen[...] = image
        wide = (rows, LANES)
        scale[1] = jnp.broadcast_to(ratio, wide)
        scale[2] = jnp.broadcast_to(length, wide)
        scale[3] = jnp.broadcast_to(norm, wide)
        square = jnp.broadcast_to(row_sums(image * image), wide)
        stat[p] = square
        stat_land[p, row] = square

        @pl.loop(1, nr)
        def _(s):
            row_copy(p, s).start()

    def phase(p):
        b = lax.rem(p, 2)

        def reduced(j, a):
            part_copy(j, a).wait()
            part[j, core, a] = part[j, core, a] + part_land[j, a]

        def rightward(j, a):
            @pl.when(z > 0)
            def _():
                right_copy(b, j, a).wait_recv()

            @pl.when(z < last_z)
            def _():
                right_out[j, a] = right_in[b, j, a] + part[j, core, a]
                right_copy(b, j, a).start()

        def leftward(j, a):
            @pl.when(z < last_z)
            def _():
                left_copy(b, j, a).wait_recv()

            @pl.when(z > 0)
            def _():
                left_out[j, a] = left_in[b, j, a] + part[j, core, a]
                left_copy(b, j, a).start()

        def joined(j, a):
            total[j, core, a] = (right_in[b, j, a] + part[j, core, a]) + left_in[b, j, a]
            total_copy(j, a, core).start()

        def spread_back(j):
            cols = columns(j)
            top, rest = halves(seen[...])
            both = dot(jnp.concatenate([top, rest], axis=0), high[:, cols], ((1,), (0,)))
            values = both[:rows] + (both[rows:] + dot(top, low[:, cols], ((1,), (0,))))
            for side in range(2):
                for a in range(PARTS):
                    at = side * half + a * piece
                    part[j, side, a] = values[:, at:at + piece]

            @pl.when(p == 0)
            def _():
                held = direct[:, cols]
                for side in range(2):
                    for a in range(PARTS):
                        at = side * half + a * piece
                        part[j, side, a] += held[:, at:at + piece]

            for a in range(PARTS):
                part_copy(j, a).start()

        def product(j):
            for a in range(PARTS):
                total_copy(j, a, core).wait_send()
                total_copy(j, a, other).wait_recv()

                @pl.when(z < last_z)
                def _():
                    right_copy(b, j, a).wait_send()

                @pl.when(z > 0)
                def _():
                    left_copy(b, j, a).wait_send()

            cols = columns(j)
            image = jnp.concatenate(
                [total[j, side, a] for side in range(2) for a in range(PARTS)], axis=1
            )
            kept = jnp.where(p == 0, 0.0, 1.0)
            before = resid[:, cols] * kept
            along = before + scale[1][:, :1] * direct[:, cols]
            after = before - scale[0][:, :1] * (image + penalty * along)
            resid[:, cols] = after
            direct[:, cols] = along

            @pl.when(j == 0)
            def _():
                norms[...] = jnp.zeros_like(norms)
                acc[...] = jnp.zeros_like(acc)

            norms[0] += lane_sums(after * after)
            norms[1] += lane_sums(after * along)
            top, rest = halves(after)
            acc[: 2 * rows] += dot(
                jnp.concatenate([top, rest], axis=0), high[:, cols], ((1,), (1,))
            )
            acc[2 * rows:] += dot(top, low[:, cols], ((1,), (1,)))

        @pl.loop(0, chunks + reach)
        def _(i):
            def task(delay, body, *more):
                j = i - delay

                @pl.when(jnp.logical_and(j >= 0, j < chunks))
                def _():
                    body(j, *more)

            def relays(a):
                task(1, reduced, a)
                task(1 + HOP * z, rightward, a)
                task(1 + HOP * (last_z - z), leftward, a)
                task(1 + HOP * jnp.maximum(z, last_z - z), joined, a)

            @pl.when(jnp.logical_and(p > 0, i == SHARE))
            def _():
                out_ref[...] += step_size(p - 1)

            relays(0)
            task(0, spread_back)
            for a in range(1, PARTS):
                relays(a)
            task(reach, product)

        lane = lax.broadcasted_iota(jnp.int32, (rows, LANES), 1)
        send_cols(p, jnp.where(lane < LANES // 2, row_sums(norms[0]), row_sums(norms[1])))
        gathered(p)

    pl.loop(0, STEPS)(phase)
    step_ref[...] = step_size(STEPS - 1)


def solution(mesh):
    nr, nc = mesh.shape["row"], mesh.shape["col"]
    line = nr // 2

    def solve(design, targets, x, sparse, dual):
        depth, features = design.shape
        rows, width = x.shape
        chunks = min(CHUNKS, features // (2 * PARTS * LANES))
        half = features // chunks // 2
        vmem = pl.BlockSpec(memory_space=pltpu.VMEM)
        hbm = pl.BlockSpec(memory_space=pl.ANY)
        f32 = jnp.float32
        dma = pltpu.SemaphoreType.DMA
        one, two = (PARTS, rows, half // PARTS), (2, PARTS, rows, half // PARTS)
        result = jax.ShapeDtypeStruct((rows, width), f32)
        return pl.pallas_call(
            functools.partial(admm_kernel, nr, nc, chunks),
            out_shape=(result, result),
            in_specs=[hbm, vmem, vmem, vmem, vmem],
            out_specs=(vmem, vmem),
            scratch_shapes=[
                pltpu.VMEM((depth, features), jnp.bfloat16),
                pltpu.VMEM((depth, features), jnp.bfloat16),
                pltpu.VMEM((2, depth, width // 2), f32),
                pltpu.VMEM((rows, features), f32),
                pltpu.VMEM((rows, features), f32),
                pltpu.VMEM((rows, depth), f32),
                pltpu.VMEM((3 * rows, depth), f32),
                pltpu.VMEM((2, rows, LANES), f32),
                pltpu.VMEM((4, rows, LANES), f32),
                pltpu.VMEM((chunks,) + two, f32),
                pltpu.VMEM((chunks,) + one, f32),
                pltpu.VMEM((2, chunks) + one, f32),
                pltpu.VMEM((2, chunks) + one, f32),
                pltpu.VMEM((chunks,) + one, f32),
                pltpu.VMEM((chunks,) + one, f32),
                pltpu.VMEM((chunks,) + two, f32),
                pltpu.VMEM((STEPS + 1, rows, depth + LANES), f32),
                pltpu.VMEM((STEPS + 1, nc, rows, depth + LANES), f32),
                pltpu.VMEM((STEPS, rows, LANES), f32),
                pltpu.VMEM((STEPS, nr, rows, LANES), f32),
                dma((2,)),
                dma((line + 2, 2)),
                dma((line, 2)),
                dma((line, 2)),
                dma((line, 2)),
            ] + [dma((chunks, PARTS))] * 4 + [
                dma((chunks, PARTS)),
                dma((2, chunks, PARTS)),
                dma((chunks, PARTS)),
                dma((2, chunks, PARTS)),
                dma((STEPS + 1, nc)),
                dma((STEPS + 1, nc)),
                dma((STEPS, nr)),
                dma((STEPS, nr)),
            ],
            compiler_params=pltpu.CompilerParams(
                collective_id=0, has_side_effects=True, vmem_limit_bytes=VMEM_LIMIT
            ),
        )(design, targets, x, sparse, dual)

    def on_device(design, targets, warm_solution, warm_sparse, warm_dual, sparsity):
        reached, step = solve(design, targets, warm_solution, warm_sparse, warm_dual)
        thresh = (sparsity / penalty)[:, None]
        solution = reached + step
        merged = solution + warm_dual
        sparse = jnp.sign(merged) * jnp.maximum(jnp.abs(merged) - thresh, 0.0)
        return solution, sparse, merged - sparse

    vector = P(None, ("col", "row"))
    return jax.shard_map(
        on_device,
        mesh=mesh,
        in_specs=(P("row", "col"), P(None, "row"), vector, vector, vector, P()),
        out_specs=(vector, vector, vector),
        check_vma=False,
    )
```

```python
import functools

import jax
import jax.numpy as jnp
from jax import lax
from jax.experimental import pallas as pl
from jax.experimental.pallas import tpu as pltpu
from jax.sharding import PartitionSpec as P

STEPS = 3
CHUNKS = 16
PARTS = 2
HOP = 2
SHARE = 3
LANES = 128
BLOCK = 256
VMEM_LIMIT = 60 * 1024 * 1024
MESH = pl.DeviceIdType.MESH

penalty = 0.5


def halves(values):
    top = values.astype(jnp.bfloat16)
    return top, (values - top.astype(jnp.float32)).astype(jnp.bfloat16)


def dot(left, right, dims):
    return lax.dot_general(left, right, (dims, ((), ())), preferred_element_type=jnp.float32)


def lane_sums(values):
    total = values[:, :LANES]
    for at in range(LANES, values.shape[1], LANES):
        total = total + values[:, at:at + LANES]
    return total


def row_sums(values):
    return jnp.sum(values, axis=1, keepdims=True)


def admm_kernel(
    nr, nc, chunks,
    design_ref, targets_ref, x_ref, sparse_ref, dual_ref, out_ref, step_ref,
    high, low, stage, resid, direct, seen, acc, norms, scale,
    part, part_land, right_in, left_in, right_out, left_out, total,
    mine, land, note, note_land, stat, stat_land,
    load_sem, gather_send, gather_recv, across_send, across_recv,
    part_send, part_recv, total_send, total_recv,
    right_send, right_recv, left_send, left_recv,
    col_send, col_recv, note_send, note_recv, row_send, row_recv,
):
    row, col = lax.axis_index("row"), lax.axis_index("col")
    line = nr // 2
    z, core = row // 2, row % 2
    other = 1 - core
    depth, features = high.shape
    rows, width = x_ref.shape
    chunk = features // chunks
    half = chunk // 2
    piece = half // PARTS
    bit = width // 2
    last_z = line - 1
    reach = 2 + HOP * last_z

    def own(slot):
        return pl.ds(pl.multiple_of(slot * width, LANES), width)

    def bits(slot, h):
        return pl.ds(pl.multiple_of(slot * width + h * bit, LANES), bit)

    def remote(source, target, send, recv, where):
        return pltpu.make_async_remote_copy(
            src_ref=source, dst_ref=target, send_sem=send, recv_sem=recv,
            device_id=where, device_id_type=MESH,
        )

    near = jnp.minimum(z, last_z - z)
    far_sign = jnp.where(z < last_z - z, 1, -1)

    def origin_at(k):
        paired = k <= 2 * near
        distance = jnp.where(paired, (k + 1) // 2, k - near)
        sign = jnp.where(paired, 1 - 2 * (k % 2), far_sign)
        return z + sign * distance, sign

    def piece_at(n):
        origin, _ = origin_at(n // 4)
        return bits(origin * 2 + jnp.where(n % 2 == 0, core, other), (n // 2) % 2)

    def load(n):
        buffer = n % 2
        return pltpu.make_async_copy(
            design_ref.at[:, piece_at(n)], stage.at[buffer], load_sem.at[buffer]
        )

    def along_line(source, origin, h, sign, at):
        return remote(
            source, resid.at[:, bits(origin * 2 + core, h)], gather_send.at[at, h],
            gather_recv.at[origin, h], {"row": (z + sign) * 2 + core},
        )

    def across(source, origin, h):
        return remote(
            source, resid.at[:, bits(origin * 2 + core, h)], across_send.at[origin, h],
            across_recv.at[origin, h], {"row": z * 2 + other},
        )

    def arrived(origin, h):
        where = resid.at[:, bits(origin * 2 + other, h)]
        return remote(
            where, where, across_send.at[origin, h], across_recv.at[origin, h],
            {"row": z * 2 + other},
        )

    def inside(place):
        return jnp.logical_and(place >= 0, place < line)

    load(0).start()
    load(1).start()

    barrier = pltpu.get_barrier_semaphore()

    @pl.loop(1, nc)
    def _(s):
        pl.semaphore_signal(
            barrier, inc=1, device_id={"col": lax.rem(col + s, nc)}, device_id_type=MESH
        )

    @pl.loop(1, nr)
    def _(s):
        pl.semaphore_signal(
            barrier, inc=1, device_id={"row": lax.rem(row + s, nr)}, device_id_type=MESH
        )

    resid[:, own(row)] = x_ref[...]
    out_ref[...] = x_ref[...]
    direct[...] = jnp.zeros_like(direct)
    direct[:, own(row)] = penalty * ((sparse_ref[...] - dual_ref[...]) - x_ref[...])
    acc[...] = jnp.zeros_like(acc)
    note[...] = jnp.zeros_like(note)
    scale[0] = jnp.full_like(scale[0], -1.0)
    for i in range(1, 4):
        scale[i] = jnp.zeros_like(scale[i])

    @pl.when(z == 0)
    def _():
        right_in[...] = jnp.zeros_like(right_in)

    @pl.when(z == last_z)
    def _():
        left_in[...] = jnp.zeros_like(left_in)

    pl.semaphore_wait(barrier, nc + nr - 2)

    for h in range(2):
        source = x_ref.at[:, pl.ds(h * bit, bit)]
        for i, sign in enumerate((1, -1)):

            @pl.when(inside(z + sign))
            def _():
                along_line(source, z, h, sign, line + i).start()

        across(source, z, h).start()

    def relay(distance, h):
        for sign in (1, -1):
            origin = z + sign * distance

            @pl.when(inside(origin))
            def _():
                held = resid.at[:, bits(origin * 2 + core, h)]
                along_line(held, origin, h, sign, origin).wait_recv()

                @pl.when(inside(z - sign))
                def _():
                    along_line(held, origin, h, -sign, origin).start()

                across(held, origin, h).start()

    @pl.loop(0, 2 * nr)
    def _(n):
        @pl.when(jnp.logical_and(n >= 4, n % 2 == 0))
        def _():
            relay(n // 4, (n // 2) % 2)

        load(n).wait()

        @pl.when(n % 2 == 1)
        def _():
            arrived(origin_at(n // 4)[0], (n // 2) % 2).wait_recv()

        cols = piece_at(n)
        top, rest = halves(resid[:, cols])
        both = jnp.concatenate([top, rest], axis=0)
        for at in range(0, depth, BLOCK):
            design_top, design_rest = halves(stage[n % 2, at:at + BLOCK])
            high[at:at + BLOCK, cols] = design_top
            low[at:at + BLOCK, cols] = design_rest
            acc[: 2 * rows, at:at + BLOCK] += dot(both, design_top, ((1,), (1,)))
            acc[2 * rows:, at:at + BLOCK] += dot(top, design_rest, ((1,), (1,)))

        @pl.when(n + 2 < 2 * nr)
        def _():
            load(n + 2).start()

    @pl.loop(0, line)
    def _(k):
        origin, sign = origin_at(k)
        for h in range(2):
            source = x_ref.at[:, pl.ds(h * bit, bit)]
            across(source, origin, h).wait_send()

            @pl.when(jnp.logical_and(k > 0, inside(z - sign)))
            def _():
                along_line(source, origin, h, -sign, origin).wait_send()

    for h in range(2):
        source = x_ref.at[:, pl.ds(h * bit, bit)]
        for i, sign in enumerate((1, -1)):

            @pl.when(inside(z + sign))
            def _():
                along_line(source, z, h, sign, line + i).wait_send()

    def to_cols(slot, s):
        return remote(
            mine.at[slot], land.at[slot, col], col_send.at[slot, s], col_recv.at[slot, s],
            {"col": lax.rem(col + s, nc)},
        )

    def note_copy(p, s):
        return remote(
            note.at[p], note_land.at[p, col], note_send.at[p, s], note_recv.at[p, s],
            {"col": lax.rem(col + s, nc)},
        )

    def summed(slot):
        @pl.loop(1, nc)
        def _(s):
            to_cols(slot, s).wait()

        values = land[slot, 0]
        for s in range(1, nc):
            values = values + land[slot, s]
        return values

    def send_cols(slot):
        mine[slot] = acc[:rows] + (acc[rows:2 * rows] + acc[2 * rows:])

        @pl.loop(1, nc)
        def _(s):
            to_cols(slot, s).start()

        land[slot, col] = mine[slot]

    send_cols(STEPS)
    seen[...] = targets_ref[...] - summed(STEPS)

    def pair(source, target, send, recv):
        return remote(source, target, send, recv, {"row": z * 2 + other})

    def part_copy(j, a):
        return pair(
            part.at[j, other, a], part_land.at[j, a],
            part_send.at[j, a], part_recv.at[j, a],
        )

    def total_copy(j, a, side):
        where = total.at[j, side, a]
        return pair(where, where, total_send.at[j, a], total_recv.at[j, a])

    def right_copy(b, j, a):
        return remote(
            right_out.at[j, a], right_in.at[b, j, a],
            right_send.at[j, a], right_recv.at[b, j, a], {"row": (z + 1) * 2 + core},
        )

    def left_copy(b, j, a):
        return remote(
            left_out.at[j, a], left_in.at[b, j, a],
            left_send.at[j, a], left_recv.at[b, j, a], {"row": (z - 1) * 2 + core},
        )

    def row_copy(p, s):
        return remote(
            stat.at[p], stat_land.at[p, row], row_send.at[p, s], row_recv.at[p, s],
            {"row": lax.rem(row + s, nr)},
        )

    def columns(j):
        return pl.ds(pl.multiple_of(j * chunk, LANES), chunk)

    def step_size(p):
        @pl.loop(1, nr)
        def _(s):
            row_copy(p, s).wait()

        square = stat_land[p, 0]
        for s in range(1, nr):
            square = square + stat_land[p, s]
        alpha = scale[3] / (square + penalty * scale[2])
        scale[0] = alpha
        along = resid[:, own(row)] + scale[1][:, :1] * direct[:, own(row)]
        return alpha[:, :1] * along

    def gathered(p):
        values = summed(p)

        @pl.loop(1, nc)
        def _(s):
            note_copy(p, s).wait()

        told = note_land[p, 0]
        for s in range(1, nc):
            told = told + note_land[p, s]
        told = jnp.transpose(told)[:rows]
        norm, cross = told[:, :1], told[:, 7:8]
        start = p == 0
        before = jnp.where(start, norm, scale[3][:, :1])
        ratio = jnp.where(start, 0.0, norm / before)
        length = norm + ratio * (2.0 * cross + ratio * scale[2][:, :1])
        image = values + ratio * seen[...]
        seen[...] = image
        wide = (rows, LANES)
        scale[1] = jnp.broadcast_to(ratio, wide)
        scale[2] = jnp.broadcast_to(length, wide)
        scale[3] = jnp.broadcast_to(norm, wide)
        square = jnp.broadcast_to(row_sums(image * image), wide)
        stat[p] = square
        stat_land[p, row] = square

        @pl.loop(1, nr)
        def _(s):
            row_copy(p, s).start()

    def phase(p):
        b = lax.rem(p, 2)

        def reduced(j, a):
            part_copy(j, a).wait()
            part[j, core, a] = part[j, core, a] + part_land[j, a]

        def rightward(j, a):
            @pl.when(z > 0)
            def _():
                right_copy(b, j, a).wait_recv()

            @pl.when(z < last_z)
            def _():
                right_out[j, a] = right_in[b, j, a] + part[j, core, a]
                right_copy(b, j, a).start()

        def leftward(j, a):
            @pl.when(z < last_z)
            def _():
                left_copy(b, j, a).wait_recv()

            @pl.when(z > 0)
            def _():
                left_out[j, a] = left_in[b, j, a] + part[j, core, a]
                left_copy(b, j, a).start()

        def joined(j, a):
            total[j, core, a] = (right_in[b, j, a] + part[j, core, a]) + left_in[b, j, a]
            total_copy(j, a, core).start()

        def spread_back(j):
            cols = columns(j)
            top, rest = halves(seen[...])
            both = dot(jnp.concatenate([top, rest], axis=0), high[:, cols], ((1,), (0,)))
            values = both[:rows] + (both[rows:] + dot(top, low[:, cols], ((1,), (0,))))
            for side in range(2):
                for a in range(PARTS):
                    at = side * half + a * piece
                    part[j, side, a] = values[:, at:at + piece]

            @pl.when(p == 0)
            def _():
                held = direct[:, cols]
                for side in range(2):
                    for a in range(PARTS):
                        at = side * half + a * piece
                        part[j, side, a] += held[:, at:at + piece]

            for a in range(PARTS):
                part_copy(j, a).start()

        def product(j):
            for a in range(PARTS):
                total_copy(j, a, core).wait_send()
                total_copy(j, a, other).wait_recv()

                @pl.when(z < last_z)
                def _():
                    right_copy(b, j, a).wait_send()

                @pl.when(z > 0)
                def _():
                    left_copy(b, j, a).wait_send()

            cols = columns(j)
            image = jnp.concatenate(
                [total[j, side, a] for side in range(2) for a in range(PARTS)], axis=1
            )
            kept = jnp.where(p == 0, 0.0, 1.0)
            before = resid[:, cols] * kept
            along = before + scale[1][:, :1] * direct[:, cols]
            after = before - scale[0][:, :1] * (image + penalty * along)
            resid[:, cols] = after
            direct[:, cols] = along

            @pl.when(j == 0)
            def _():
                norms[...] = jnp.zeros_like(norms)
                acc[...] = jnp.zeros_like(acc)

            norms[0] += lane_sums(after * after)
            norms[1] += lane_sums(after * along)
            top, rest = halves(after)
            acc[: 2 * rows] += dot(
                jnp.concatenate([top, rest], axis=0), high[:, cols], ((1,), (1,))
            )
            acc[2 * rows:] += dot(top, low[:, cols], ((1,), (1,)))

        @pl.loop(0, chunks + reach)
        def _(i):
            def task(delay, body, *more):
                j = i - delay

                @pl.when(jnp.logical_and(j >= 0, j < chunks))
                def _():
                    body(j, *more)

            def relays(a):
                task(1, reduced, a)
                task(1 + HOP * z, rightward, a)
                task(1 + HOP * (last_z - z), leftward, a)
                task(1 + HOP * jnp.maximum(z, last_z - z), joined, a)

            @pl.when(jnp.logical_and(p > 0, i == SHARE))
            def _():
                out_ref[...] += step_size(p - 1)

            relays(0)
            task(0, spread_back)
            for a in range(1, PARTS):
                relays(a)
            task(reach, product)

        send_cols(p)
        lane = lax.broadcasted_iota(jnp.int32, (rows, LANES), 1)
        told = jnp.where(lane < 4, row_sums(norms[0]), row_sums(norms[1]))
        note[p, :, :rows] = jnp.transpose(told)[:8]

        @pl.loop(1, nc)
        def _(s):
            note_copy(p, s).start()

        note_land[p, col] = note[p]
        gathered(p)

    pl.loop(0, STEPS)(phase)
    step_ref[...] = step_size(STEPS - 1)


def solution(mesh):
    nr, nc = mesh.shape["row"], mesh.shape["col"]
    line = nr // 2

    def solve(design, targets, x, sparse, dual):
        depth, features = design.shape
        rows, width = x.shape
        chunks = min(CHUNKS, features // (2 * PARTS * LANES))
        half = features // chunks // 2
        vmem = pl.BlockSpec(memory_space=pltpu.VMEM)
        hbm = pl.BlockSpec(memory_space=pl.ANY)
        f32 = jnp.float32
        dma = pltpu.SemaphoreType.DMA
        one, two = (PARTS, rows, half // PARTS), (2, PARTS, rows, half // PARTS)
        result = jax.ShapeDtypeStruct((rows, width), f32)
        return pl.pallas_call(
            functools.partial(admm_kernel, nr, nc, chunks),
            out_shape=(result, result),
            in_specs=[hbm, vmem, vmem, vmem, vmem],
            out_specs=(vmem, vmem),
            scratch_shapes=[
                pltpu.VMEM((depth, features), jnp.bfloat16),
                pltpu.VMEM((depth, features), jnp.bfloat16),
                pltpu.VMEM((2, depth, width // 2), f32),
                pltpu.VMEM((rows, features), f32),
                pltpu.VMEM((rows, features), f32),
                pltpu.VMEM((rows, depth), f32),
                pltpu.VMEM((3 * rows, depth), f32),
                pltpu.VMEM((2, rows, LANES), f32),
                pltpu.VMEM((4, rows, LANES), f32),
                pltpu.VMEM((chunks,) + two, f32),
                pltpu.VMEM((chunks,) + one, f32),
                pltpu.VMEM((2, chunks) + one, f32),
                pltpu.VMEM((2, chunks) + one, f32),
                pltpu.VMEM((chunks,) + one, f32),
                pltpu.VMEM((chunks,) + one, f32),
                pltpu.VMEM((chunks,) + two, f32),
                pltpu.VMEM((STEPS + 1, rows, depth), f32),
                pltpu.VMEM((STEPS + 1, nc, rows, depth), f32),
                pltpu.VMEM((STEPS, 8, LANES), f32),
                pltpu.VMEM((STEPS, nc, 8, LANES), f32),
                pltpu.VMEM((STEPS, rows, LANES), f32),
                pltpu.VMEM((STEPS, nr, rows, LANES), f32),
                dma((2,)),
                dma((line + 2, 2)),
                dma((line, 2)),
                dma((line, 2)),
                dma((line, 2)),
            ] + [dma((chunks, PARTS))] * 4 + [
                dma((chunks, PARTS)),
                dma((2, chunks, PARTS)),
                dma((chunks, PARTS)),
                dma((2, chunks, PARTS)),
                dma((STEPS + 1, nc)),
                dma((STEPS + 1, nc)),
                dma((STEPS, nc)),
                dma((STEPS, nc)),
                dma((STEPS, nr)),
                dma((STEPS, nr)),
            ],
            compiler_params=pltpu.CompilerParams(
                collective_id=0, has_side_effects=True, vmem_limit_bytes=VMEM_LIMIT
            ),
        )(design, targets, x, sparse, dual)

    def on_device(design, targets, warm_solution, warm_sparse, warm_dual, sparsity):
        reached, step = solve(design, targets, warm_solution, warm_sparse, warm_dual)
        thresh = (sparsity / penalty)[:, None]
        solution = reached + step
        merged = solution + warm_dual
        sparse = jnp.sign(merged) * jnp.maximum(jnp.abs(merged) - thresh, 0.0)
        return solution, sparse, merged - sparse

    vector = P(None, ("col", "row"))
    return jax.shard_map(
        on_device,
        mesh=mesh,
        in_specs=(P("row", "col"), P(None, "row"), vector, vector, vector, P()),
        out_specs=(vector, vector, vector),
        check_vma=False,
    )
```

```python
import functools

import jax
import jax.numpy as jnp
from jax import lax
from jax.experimental import pallas as pl
from jax.experimental.pallas import tpu as pltpu
from jax.sharding import PartitionSpec as P

STEPS = 3
CHUNKS = 16
PARTS = 2
HOP = 2
SHARE = 6
LANES = 128
BLOCK = 256
VMEM_LIMIT = 60 * 1024 * 1024
MESH = pl.DeviceIdType.MESH

penalty = 0.5


def halves(values):
    top = values.astype(jnp.bfloat16)
    return top, (values - top.astype(jnp.float32)).astype(jnp.bfloat16)


def dot(left, right, dims):
    return lax.dot_general(left, right, (dims, ((), ())), preferred_element_type=jnp.float32)


def lane_sums(values):
    total = values[:, :LANES]
    for at in range(LANES, values.shape[1], LANES):
        total = total + values[:, at:at + LANES]
    return total


def row_sums(values):
    return jnp.sum(values, axis=1, keepdims=True)


def admm_kernel(
    nr, nc, chunks,
    design_ref, targets_ref, x_ref, sparse_ref, dual_ref, out_ref, step_ref,
    high, low, stage, resid, direct, seen, acc, norms, scale,
    part, part_land, right_in, left_in, right_out, left_out, total,
    mine, land, note, note_land, stat, stat_land,
    load_sem, gather_send, gather_recv, across_send, across_recv,
    part_send, part_recv, total_send, total_recv,
    right_send, right_recv, left_send, left_recv,
    col_send, col_recv, note_send, note_recv, row_send, row_recv,
):
    row, col = lax.axis_index("row"), lax.axis_index("col")
    line = nr // 2
    z, core = row // 2, row % 2
    other = 1 - core
    depth, features = high.shape
    rows, width = x_ref.shape
    chunk = features // chunks
    half = chunk // 2
    piece = half // PARTS
    bit = width // 2
    last_z = line - 1
    reach = 2 + HOP * last_z

    def own(slot):
        return pl.ds(pl.multiple_of(slot * width, LANES), width)

    def bits(slot, h):
        return pl.ds(pl.multiple_of(slot * width + h * bit, LANES), bit)

    def remote(source, target, send, recv, where):
        return pltpu.make_async_remote_copy(
            src_ref=source, dst_ref=target, send_sem=send, recv_sem=recv,
            device_id=where, device_id_type=MESH,
        )

    near = jnp.minimum(z, last_z - z)
    far_sign = jnp.where(z < last_z - z, 1, -1)

    def origin_at(k):
        paired = k <= 2 * near
        distance = jnp.where(paired, (k + 1) // 2, k - near)
        sign = jnp.where(paired, 1 - 2 * (k % 2), far_sign)
        return z + sign * distance, sign

    def piece_at(n):
        origin, _ = origin_at(n // 4)
        return bits(origin * 2 + jnp.where(n % 2 == 0, core, other), (n // 2) % 2)

    def load(n):
        buffer = n % 2
        return pltpu.make_async_copy(
            design_ref.at[:, piece_at(n)], stage.at[buffer], load_sem.at[buffer]
        )

    def along_line(source, origin, h, sign, at):
        return remote(
            source, resid.at[:, bits(origin * 2 + core, h)], gather_send.at[at, h],
            gather_recv.at[origin, h], {"row": (z + sign) * 2 + core},
        )

    def across(source, origin, h):
        return remote(
            source, resid.at[:, bits(origin * 2 + core, h)], across_send.at[origin, h],
            across_recv.at[origin, h], {"row": z * 2 + other},
        )

    def arrived(origin, h):
        where = resid.at[:, bits(origin * 2 + other, h)]
        return remote(
            where, where, across_send.at[origin, h], across_recv.at[origin, h],
            {"row": z * 2 + other},
        )

    def inside(place):
        return jnp.logical_and(place >= 0, place < line)

    load(0).start()
    load(1).start()

    barrier = pltpu.get_barrier_semaphore()

    @pl.loop(1, nc)
    def _(s):
        pl.semaphore_signal(
            barrier, inc=1, device_id={"col": lax.rem(col + s, nc)}, device_id_type=MESH
        )

    @pl.loop(1, nr)
    def _(s):
        pl.semaphore_signal(
            barrier, inc=1, device_id={"row": lax.rem(row + s, nr)}, device_id_type=MESH
        )

    resid[:, own(row)] = x_ref[...]
    out_ref[...] = x_ref[...]
    direct[...] = jnp.zeros_like(direct)
    direct[:, own(row)] = penalty * ((sparse_ref[...] - dual_ref[...]) - x_ref[...])
    acc[...] = jnp.zeros_like(acc)
    note[...] = jnp.zeros_like(note)
    scale[0] = jnp.full_like(scale[0], -1.0)
    for i in range(1, 4):
        scale[i] = jnp.zeros_like(scale[i])

    @pl.when(z == 0)
    def _():
        right_in[...] = jnp.zeros_like(right_in)

    @pl.when(z == last_z)
    def _():
        left_in[...] = jnp.zeros_like(left_in)

    pl.semaphore_wait(barrier, nc + nr - 2)

    for h in range(2):
        source = x_ref.at[:, pl.ds(h * bit, bit)]
        for i, sign in enumerate((1, -1)):

            @pl.when(inside(z + sign))
            def _():
                along_line(source, z, h, sign, line + i).start()

        across(source, z, h).start()

    def relay(distance, h):
        for sign in (1, -1):
            origin = z + sign * distance

            @pl.when(inside(origin))
            def _():
                held = resid.at[:, bits(origin * 2 + core, h)]
                along_line(held, origin, h, sign, origin).wait_recv()

                @pl.when(inside(z - sign))
                def _():
                    along_line(held, origin, h, -sign, origin).start()

                across(held, origin, h).start()

    @pl.loop(0, 2 * nr)
    def _(n):
        @pl.when(jnp.logical_and(n >= 4, n % 2 == 0))
        def _():
            relay(n // 4, (n // 2) % 2)

        load(n).wait()

        @pl.when(n % 2 == 1)
        def _():
            arrived(origin_at(n // 4)[0], (n // 2) % 2).wait_recv()

        cols = piece_at(n)
        top, rest = halves(resid[:, cols])
        both = jnp.concatenate([top, rest], axis=0)
        for at in range(0, depth, BLOCK):
            design_top, design_rest = halves(stage[n % 2, at:at + BLOCK])
            high[at:at + BLOCK, cols] = design_top
            low[at:at + BLOCK, cols] = design_rest
            acc[: 2 * rows, at:at + BLOCK] += dot(both, design_top, ((1,), (1,)))
            acc[2 * rows:, at:at + BLOCK] += dot(top, design_rest, ((1,), (1,)))

        @pl.when(n + 2 < 2 * nr)
        def _():
            load(n + 2).start()

    @pl.loop(0, line)
    def _(k):
        origin, sign = origin_at(k)
        for h in range(2):
            source = x_ref.at[:, pl.ds(h * bit, bit)]
            across(source, origin, h).wait_send()

            @pl.when(jnp.logical_and(k > 0, inside(z - sign)))
            def _():
                along_line(source, origin, h, -sign, origin).wait_send()

    for h in range(2):
        source = x_ref.at[:, pl.ds(h * bit, bit)]
        for i, sign in enumerate((1, -1)):

            @pl.when(inside(z + sign))
            def _():
                along_line(source, z, h, sign, line + i).wait_send()

    def to_cols(slot, s):
        return remote(
            mine.at[slot], land.at[slot, col], col_send.at[slot, s], col_recv.at[slot, s],
            {"col": lax.rem(col + s, nc)},
        )

    def note_copy(p, s):
        return remote(
            note.at[p], note_land.at[p, col], note_send.at[p, s], note_recv.at[p, s],
            {"col": lax.rem(col + s, nc)},
        )

    def summed(slot):
        @pl.loop(1, nc)
        def _(s):
            to_cols(slot, s).wait()

        values = land[slot, 0]
        for s in range(1, nc):
            values = values + land[slot, s]
        return values

    def send_cols(slot):
        mine[slot] = acc[:rows] + (acc[rows:2 * rows] + acc[2 * rows:])

        @pl.loop(1, nc)
        def _(s):
            to_cols(slot, s).start()

        land[slot, col] = mine[slot]

    send_cols(STEPS)
    seen[...] = targets_ref[...] - summed(STEPS)

    def pair(source, target, send, recv):
        return remote(source, target, send, recv, {"row": z * 2 + other})

    def part_copy(j, a):
        return pair(
            part.at[j, other, a], part_land.at[j, a],
            part_send.at[j, a], part_recv.at[j, a],
        )

    def total_copy(j, a, side):
        where = total.at[j, side, a]
        return pair(where, where, total_send.at[j, a], total_recv.at[j, a])

    def right_copy(b, j, a):
        return remote(
            right_out.at[j, a], right_in.at[b, j, a],
            right_send.at[j, a], right_recv.at[b, j, a], {"row": (z + 1) * 2 + core},
        )

    def left_copy(b, j, a):
        return remote(
            left_out.at[j, a], left_in.at[b, j, a],
            left_send.at[j, a], left_recv.at[b, j, a], {"row": (z - 1) * 2 + core},
        )

    def row_copy(p, s):
        return remote(
            stat.at[p], stat_land.at[p, row], row_send.at[p, s], row_recv.at[p, s],
            {"row": lax.rem(row + s, nr)},
        )

    def columns(j):
        return pl.ds(pl.multiple_of(j * chunk, LANES), chunk)

    def step_size(p):
        @pl.loop(1, nr)
        def _(s):
            row_copy(p, s).wait()

        square = stat_land[p, 0]
        for s in range(1, nr):
            square = square + stat_land[p, s]
        alpha = scale[3] / (square + penalty * scale[2])
        scale[0] = alpha
        along = resid[:, own(row)] + scale[1][:, :1] * direct[:, own(row)]
        return alpha[:, :1] * along

    def gathered(p):
        values = summed(p)

        @pl.loop(1, nc)
        def _(s):
            note_copy(p, s).wait()

        told = note_land[p, 0]
        for s in range(1, nc):
            told = told + note_land[p, s]
        told = jnp.transpose(told)[:rows]
        norm, cross = told[:, :1], told[:, 7:8]
        start = p == 0
        before = jnp.where(start, norm, scale[3][:, :1])
        ratio = jnp.where(start, 0.0, norm / before)
        length = norm + ratio * (2.0 * cross + ratio * scale[2][:, :1])
        image = values + ratio * seen[...]
        seen[...] = image
        wide = (rows, LANES)
        scale[1] = jnp.broadcast_to(ratio, wide)
        scale[2] = jnp.broadcast_to(length, wide)
        scale[3] = jnp.broadcast_to(norm, wide)

    def share(p):
        image = seen[...]
        square = jnp.broadcast_to(row_sums(image * image), (rows, LANES))
        stat[p] = square
        stat_land[p, row] = square

        @pl.loop(1, nr)
        def _(s):
            row_copy(p, s).start()

    def phase(p):
        b = lax.rem(p, 2)

        def reduced(j, a):
            part_copy(j, a).wait()
            part[j, core, a] = part[j, core, a] + part_land[j, a]

        def rightward(j, a):
            @pl.when(z > 0)
            def _():
                right_copy(b, j, a).wait_recv()

            @pl.when(z < last_z)
            def _():
                right_out[j, a] = right_in[b, j, a] + part[j, core, a]
                right_copy(b, j, a).start()

        def leftward(j, a):
            @pl.when(z < last_z)
            def _():
                left_copy(b, j, a).wait_recv()

            @pl.when(z > 0)
            def _():
                left_out[j, a] = left_in[b, j, a] + part[j, core, a]
                left_copy(b, j, a).start()

        def joined(j, a):
            total[j, core, a] = (right_in[b, j, a] + part[j, core, a]) + left_in[b, j, a]
            total_copy(j, a, core).start()

        def spread_back(j):
            cols = columns(j)
            top, rest = halves(seen[...])
            both = dot(jnp.concatenate([top, rest], axis=0), high[:, cols], ((1,), (0,)))
            values = both[:rows] + (both[rows:] + dot(top, low[:, cols], ((1,), (0,))))
            for side in range(2):
                for a in range(PARTS):
                    at = side * half + a * piece
                    part[j, side, a] = values[:, at:at + piece]

            @pl.when(p == 0)
            def _():
                held = direct[:, cols]
                for side in range(2):
                    for a in range(PARTS):
                        at = side * half + a * piece
                        part[j, side, a] += held[:, at:at + piece]

            for a in range(PARTS):
                part_copy(j, a).start()

        def product(j):
            for a in range(PARTS):
                total_copy(j, a, core).wait_send()
                total_copy(j, a, other).wait_recv()

                @pl.when(z < last_z)
                def _():
                    right_copy(b, j, a).wait_send()

                @pl.when(z > 0)
                def _():
                    left_copy(b, j, a).wait_send()

            cols = columns(j)
            image = jnp.concatenate(
                [total[j, side, a] for side in range(2) for a in range(PARTS)], axis=1
            )
            kept = jnp.where(p == 0, 0.0, 1.0)
            before = resid[:, cols] * kept
            along = before + scale[1][:, :1] * direct[:, cols]
            after = before - scale[0][:, :1] * (image + penalty * along)
            resid[:, cols] = after
            direct[:, cols] = along

            @pl.when(j == 0)
            def _():
                norms[...] = jnp.zeros_like(norms)
                acc[...] = jnp.zeros_like(acc)

            norms[0] += lane_sums(after * after)
            norms[1] += lane_sums(after * along)
            top, rest = halves(after)
            acc[: 2 * rows] += dot(
                jnp.concatenate([top, rest], axis=0), high[:, cols], ((1,), (1,))
            )
            acc[2 * rows:] += dot(top, low[:, cols], ((1,), (1,)))

        @pl.loop(0, chunks + reach)
        def _(i):
            def task(delay, body, *more):
                j = i - delay

                @pl.when(jnp.logical_and(j >= 0, j < chunks))
                def _():
                    body(j, *more)

            def relays(a):
                task(1, reduced, a)
                task(1 + HOP * z, rightward, a)
                task(1 + HOP * (last_z - z), leftward, a)
                task(1 + HOP * jnp.maximum(z, last_z - z), joined, a)

            @pl.when(jnp.logical_and(p > 0, i == SHARE))
            def _():
                out_ref[...] += step_size(p - 1)

            relays(0)
            task(0, spread_back)

            @pl.when(jnp.logical_and(p > 0, i == 0))
            def _():
                share(p - 1)

            for a in range(1, PARTS):
                relays(a)
            task(reach, product)

        send_cols(p)
        lane = lax.broadcasted_iota(jnp.int32, (rows, LANES), 1)
        told = jnp.where(lane < 4, row_sums(norms[0]), row_sums(norms[1]))
        note[p, :, :rows] = jnp.transpose(told)[:8]

        @pl.loop(1, nc)
        def _(s):
            note_copy(p, s).start()

        note_land[p, col] = note[p]
        gathered(p)

    pl.loop(0, STEPS)(phase)
    share(STEPS - 1)
    step_ref[...] = step_size(STEPS - 1)


def solution(mesh):
    nr, nc = mesh.shape["row"], mesh.shape["col"]
    line = nr // 2

    def solve(design, targets, x, sparse, dual):
        depth, features = design.shape
        rows, width = x.shape
        chunks = min(CHUNKS, features // (2 * PARTS * LANES))
        half = features // chunks // 2
        vmem = pl.BlockSpec(memory_space=pltpu.VMEM)
        hbm = pl.BlockSpec(memory_space=pl.ANY)
        f32 = jnp.float32
        dma = pltpu.SemaphoreType.DMA
        one, two = (PARTS, rows, half // PARTS), (2, PARTS, rows, half // PARTS)
        result = jax.ShapeDtypeStruct((rows, width), f32)
        return pl.pallas_call(
            functools.partial(admm_kernel, nr, nc, chunks),
            out_shape=(result, result),
            in_specs=[hbm, vmem, vmem, vmem, vmem],
            out_specs=(vmem, vmem),
            scratch_shapes=[
                pltpu.VMEM((depth, features), jnp.bfloat16),
                pltpu.VMEM((depth, features), jnp.bfloat16),
                pltpu.VMEM((2, depth, width // 2), f32),
                pltpu.VMEM((rows, features), f32),
                pltpu.VMEM((rows, features), f32),
                pltpu.VMEM((rows, depth), f32),
                pltpu.VMEM((3 * rows, depth), f32),
                pltpu.VMEM((2, rows, LANES), f32),
                pltpu.VMEM((4, rows, LANES), f32),
                pltpu.VMEM((chunks,) + two, f32),
                pltpu.VMEM((chunks,) + one, f32),
                pltpu.VMEM((2, chunks) + one, f32),
                pltpu.VMEM((2, chunks) + one, f32),
                pltpu.VMEM((chunks,) + one, f32),
                pltpu.VMEM((chunks,) + one, f32),
                pltpu.VMEM((chunks,) + two, f32),
                pltpu.VMEM((STEPS + 1, rows, depth), f32),
                pltpu.VMEM((STEPS + 1, nc, rows, depth), f32),
                pltpu.VMEM((STEPS, 8, LANES), f32),
                pltpu.VMEM((STEPS, nc, 8, LANES), f32),
                pltpu.VMEM((STEPS, rows, LANES), f32),
                pltpu.VMEM((STEPS, nr, rows, LANES), f32),
                dma((2,)),
                dma((line + 2, 2)),
                dma((line, 2)),
                dma((line, 2)),
                dma((line, 2)),
            ] + [dma((chunks, PARTS))] * 4 + [
                dma((chunks, PARTS)),
                dma((2, chunks, PARTS)),
                dma((chunks, PARTS)),
                dma((2, chunks, PARTS)),
                dma((STEPS + 1, nc)),
                dma((STEPS + 1, nc)),
                dma((STEPS, nc)),
                dma((STEPS, nc)),
                dma((STEPS, nr)),
                dma((STEPS, nr)),
            ],
            compiler_params=pltpu.CompilerParams(
                collective_id=0, has_side_effects=True, vmem_limit_bytes=VMEM_LIMIT
            ),
        )(design, targets, x, sparse, dual)

    def on_device(design, targets, warm_solution, warm_sparse, warm_dual, sparsity):
        reached, step = solve(design, targets, warm_solution, warm_sparse, warm_dual)
        thresh = (sparsity / penalty)[:, None]
        solution = reached + step
        merged = solution + warm_dual
        sparse = jnp.sign(merged) * jnp.maximum(jnp.abs(merged) - thresh, 0.0)
        return solution, sparse, merged - sparse

    vector = P(None, ("col", "row"))
    return jax.shard_map(
        on_device,
        mesh=mesh,
        in_specs=(P("row", "col"), P(None, "row"), vector, vector, vector, P()),
        out_specs=(vector, vector, vector),
        check_vma=False,
    )
```
